32 devices in a mesh: dp: 8 (over z, x), tensor: 4 (over y, core).
Axes of the slice: x: 2, y: 2, z: 4, core: 2. Of those that a mesh axis runs over, the one named last changes fastest.
Arguments:
- master_old: float32 [3072, 36864], P('dp', 'tensor'), may hold values from -6 to 6
- moment1_old: float32 [3072, 36864], P('dp', 'tensor'), may hold values from -4 to 4
- moment2_old: float32 [3072, 36864], P('dp', 'tensor'), may hold values from 0.0001 to 1
- grad: bfloat16 [3072, 36864], P('dp', 'tensor'), may hold values from -28 to 28
- send_slots: int32 [8, 13824], P('dp'), may hold values from 0 to 13823, each once within a row
- recv_slots: int32 [8, 13824], P('dp'), may hold values from 0 to 13823, each once within a row
Outputs:
- master_new: float32 [3072, 36864], P('dp', 'tensor')
- moment1_new: float32 [3072, 36864], P('dp', 'tensor')
- moment2_new: float32 [3072, 36864], P('dp', 'tensor')
The draws below stay inside these ranges and needn't reach their ends.
Inputs may be any that keep to these rules, and one draw needn't show every extreme that they name: `send_slots`: each row is a permutation of 0 to 13823; entry [i, j * 1728 + q] is the old slot of the q-th block that device i of dp sends to device j. `recv_slots`: each row is a permutation of 0 to 13823; entry [j, i * 1728 + q] is the new slot on device j of the q-th block from device i.
All inputs are finite; a program needn't handle non-finite values.
Results may differ from the reference program's by a relative error of at most 0.0003.
Values sent between devices are 32-bit elements; how exact they have to be, the bound alone decides.
A program may use at most 320 MiB of HBM per device.

```python
import math
import jax
import jax.numpy as jnp

ROWS = 3072
FF = 36864
SEGW = 128
RD = 384
COLS = 9216
HALF = 4608
NSEG = 36
BLK_DEV = 13824
PER_PEER = 1728
N_DP = 8
N_TENSOR = 4


def draw_grad(key, part):
    base_key = jax.random.fold_in(key, 11)
    key_base, key_column = jax.random.split(base_key, 2)
    position = jnp.arange(ROWS, dtype=jnp.float32) / (ROWS - 1)
    column_log = jax.random.uniform(key_column, (FF,), jnp.float32, -1.15, 1.15)
    column_scale = jnp.exp(column_log) / 1.465
    row_scale = jnp.power(10.0, position - 0.5) / 1.4664
    values = jax.random.truncated_normal(key_base, -6.0, 6.0, (ROWS, FF), jnp.float32)
    return (values * row_scale[:, None] * column_scale[None, :]).astype(jnp.bfloat16)


def steps_of(stream_key, shape, cuts, low, largest):
    factor_of = 1.0
    for axis_at, blocks in cuts:
        draws = jax.random.uniform(jax.random.fold_in(jax.random.fold_in(stream_key, 6), axis_at), (blocks,), jnp.float32, low / len(cuts), largest / len(cuts))
        factor_of = factor_of * jnp.repeat(jnp.exp(draws), shape[axis_at] // blocks).reshape((-1,) + (1,) * (len(shape) - 1 - axis_at))
    return factor_of


def bell_draw(rng, dims, width, most, shards=(), kind=jnp.bfloat16):
    array = width * jax.random.normal(rng, dims, jnp.float32)
    if shards:
        array = array * steps_of(rng, dims, shards, -0.22, 0.18)
    return jnp.clip(array, -most, most).astype(kind)


def setup_inputs(seed: int = 0) -> dict:
    streams_of = jax.random.split(jax.random.key(seed), 7)
    return {
        "master_old": bell_draw(streams_of[0], (ROWS, FF), 1.0, 6.0, ((0, 8), (1, 4)), jnp.float32),
        "moment1_old": bell_draw(streams_of[1], (ROWS, FF), 0.3, 4.0, ((0, 8), (1, 4)), jnp.float32),
        "moment2_old": jnp.clip(jnp.exp(math.log(1.0) - 9.2103404 * jax.random.uniform(streams_of[2], (ROWS, FF), jnp.float32) ** steps_of(streams_of[2], (ROWS, FF), ((0, 8), (1, 4)), -0.2, 0.2)), 0.0001, 1.0),
        "grad": draw_grad(jax.random.fold_in(streams_of[6], 71), 0),
        "send_slots": jax.vmap(lambda own: jax.random.permutation(own, BLK_DEV))(jax.random.split(streams_of[4], N_DP)).reshape((N_DP, BLK_DEV)).astype(jnp.int32),
        "recv_slots": jax.vmap(lambda own: jax.random.permutation(own, BLK_DEV))(jax.random.split(streams_of[5], N_DP)).reshape((N_DP, BLK_DEV)).astype(jnp.int32),
    }


beta_one = 0.9
beta_two = 0.95
correct_one = 0.6513215599
correct_two = 0.4012630608
adam_eps = 1e-08
learning_rate = 0.01
weight_decay = 0.1
clip_ratio = 0.75

def move_shard(shard, send_slots, recv_slots):
    tiles = shard.reshape(N_DP, RD, 2, NSEG, SEGW).transpose(0, 1, 3, 2, 4).reshape(N_DP, BLK_DEV, 2, SEGW)
    outgoing = jnp.take_along_axis(tiles, send_slots[:, :, None, None], axis=1)
    arrived = outgoing.reshape(N_DP, N_DP, PER_PEER, 2, SEGW).transpose(1, 0, 2, 3, 4).reshape(N_DP, BLK_DEV, 2, SEGW)
    sources = jnp.arange(N_DP, dtype=jnp.int32)[:, None]
    placed = jnp.zeros_like(arrived).at[sources, recv_slots].set(arrived)
    return placed.reshape(N_DP, RD, NSEG, 2, SEGW).transpose(0, 1, 3, 2, 4).reshape(ROWS, COLS)

def reshard(matrix, send_slots, recv_slots):
    moved = [move_shard(matrix[:, shard_index * COLS:(shard_index + 1) * COLS], send_slots, recv_slots) for shard_index in range(N_TENSOR)]
    pieces = []
    for pair_index in range(N_TENSOR // 2):
        first = moved[2 * pair_index]
        second = moved[2 * pair_index + 1]
        pieces.append(first[:, :HALF])
        pieces.append(second[:, :HALF])
        pieces.append(first[:, HALF:])
        pieces.append(second[:, HALF:])
    return jnp.concatenate(pieces, axis=1)

def reference(master_old, moment1_old, moment2_old, grad, send_slots, recv_slots):
    new_master = reshard(master_old, send_slots, recv_slots)
    new_first = reshard(moment1_old, send_slots, recv_slots)
    new_second = reshard(moment2_old, send_slots, recv_slots)
    wide = grad.astype(jnp.float32)
    sum_squares = jnp.sum(wide * wide)
    limit = clip_ratio * jnp.sqrt(jnp.float32(ROWS * FF))
    clip_scale = jnp.minimum(1.0, limit / jnp.sqrt(sum_squares + 1e-06))
    scaled = clip_scale * wide
    moment1 = beta_one * new_first + (1.0 - beta_one) * scaled
    moment2 = beta_two * new_second + (1.0 - beta_two) * scaled * scaled
    update = moment1 / correct_one / (jnp.sqrt(moment2 / correct_two) + adam_eps)
    master = new_master - learning_rate * (update + weight_decay * new_master)
    return (master, moment1, moment2)
```

```python
import jax
import jax.numpy as jnp
from jax import lax
from jax.experimental import pallas as pl
from jax.experimental.pallas import tpu as pltpu
from jax.sharding import PartitionSpec as P

ROWS = 3072
FF = 36864
SEGW = 128


beta_one = 0.9
beta_two = 0.95
correct_one = 0.6513215599
correct_two = 0.4012630608
adam_eps = 1e-08
learning_rate = 0.01
weight_decay = 0.1
clip_ratio = 0.75


def swapped(block, axis, apart):
    count = lax.axis_size(axis)
    route = []
    for low in range(count):
        high = low | 1 << apart
        if high != low and high < count:
            route += [(low, high), (high, low)]
    return lax.ppermute(block, axis, route)


VMEM_LIMIT = 60 * 1024 * 1024
UNROLL = 16


def tile_rows(matrix):
    rows, columns = matrix.shape
    return (
        matrix.reshape(rows // 8, 8, columns // SEGW, SEGW)
        .transpose(0, 2, 1, 3)
        .reshape(rows * columns // SEGW, SEGW)
    )


def from_tile_rows(lines, rows, columns):
    return (
        lines.reshape(rows // 8, columns // SEGW, 8, SEGW)
        .transpose(0, 2, 1, 3)
        .reshape(rows, columns)
    )


def line_of(slots, segments):
    row = slots // segments
    segment = slots % segments
    return (row // 8) * (2 * segments * 8) + segment * 8 + row % 8


def chunk_of(blocks):
    chunk = blocks
    for parts in (2, 4, 8):
        if blocks % (parts * UNROLL) == 0 or blocks % (parts * 8) == 0:
            chunk = blocks // parts
    return chunk


def step_of(chunk):
    return UNROLL if chunk % UNROLL == 0 else 8


def gather_kernel(lines_ref, apart_ref, x_ref, keep_ref, send_ref):
    chunk = keep_ref.shape[0]
    base = pl.program_id(0) * chunk
    keep_at = apart_ref[0]
    send_at = apart_ref[1]
    step = step_of(chunk)

    def body(i, carry):
        start = pl.multiple_of(i * step, 8)
        for k in range(step):
            line = lines_ref[base + start + k]
            keep_ref[pl.ds(start + k, 1), :] = x_ref[pl.ds(line + keep_at, 1), :]
            send_ref[pl.ds(start + k, 1), :] = x_ref[pl.ds(line + send_at, 1), :]
        return carry

    lax.fori_loop(0, chunk // step, body, 0)


def scatter_kernel(lines_ref, apart_ref, keep_ref, got_ref, out_ref):
    chunk = keep_ref.shape[0]
    base = pl.program_id(0) * chunk
    keep_at = apart_ref[0]
    got_at = apart_ref[1]
    step = step_of(chunk)

    def body(i, carry):
        start = pl.multiple_of(i * step, 8)
        for k in range(step):
            line = lines_ref[base + start + k]
            out_ref[pl.ds(line + keep_at, 1), :] = keep_ref[pl.ds(start + k, 1), :]
            out_ref[pl.ds(line + got_at, 1), :] = got_ref[pl.ds(start + k, 1), :]
        return carry

    lax.fori_loop(0, chunk // step, body, 0)


def move_call(kernel, blocks, gathering):
    chunk = chunk_of(blocks)
    whole = pl.BlockSpec((2 * blocks, SEGW), lambda i, *_: (0, 0))
    piece = pl.BlockSpec((chunk, SEGW), lambda i, *_: (i, 0))
    full = jax.ShapeDtypeStruct((2 * blocks, SEGW), jnp.float32)
    half = jax.ShapeDtypeStruct((blocks, SEGW), jnp.float32)
    return pl.pallas_call(
        kernel,
        grid_spec=pltpu.PrefetchScalarGridSpec(
            num_scalar_prefetch=2,
            grid=(blocks // chunk,),
            in_specs=[whole] if gathering else [piece, piece],
            out_specs=[piece, piece] if gathering else whole,
        ),
        out_shape=[half, half] if gathering else full,
        compiler_params=pltpu.CompilerParams(
            dimension_semantics=("arbitrary",), vmem_limit_bytes=VMEM_LIMIT
        ),
        cost_estimate=pl.CostEstimate(
            flops=0, bytes_accessed=16 * blocks * SEGW, transcendentals=0
        ),
    )


def per_device(master_old, moment1_old, moment2_old, grad, send_slots, recv_slots):
    rows_here, columns = master_old.shape
    segments = columns // 2 // SEGW
    blocks = rows_here * segments
    parity = lax.axis_index("tensor") % 2
    apart = jnp.stack([parity, 1 - parity]).astype(jnp.int32) * (segments * 8)
    send_lines = line_of(send_slots[0], segments)
    recv_lines = line_of(recv_slots[0], segments)
    gather = move_call(gather_kernel, blocks, True)
    scatter = move_call(scatter_kernel, blocks, False)

    def moved(matrix):
        keep, send = gather(send_lines, apart, tile_rows(matrix))
        got = swapped(send, "tensor", 0)
        keep = lax.all_to_all(keep, "dp", split_axis=0, concat_axis=0, tiled=True)
        got = lax.all_to_all(got, "dp", split_axis=0, concat_axis=0, tiled=True)
        return from_tile_rows(scatter(recv_lines, apart, keep, got), rows_here, columns)

    wide = grad.astype(jnp.float32)
    new_first = moved(moment1_old)
    new_second = moved(moment2_old)
    new_master = moved(master_old)
    sum_squares = lax.psum(jnp.sum(wide * wide), ("dp", "tensor"))
    limit = clip_ratio * jnp.sqrt(jnp.float32(ROWS * FF))
    clip_scale = jnp.minimum(1.0, limit / jnp.sqrt(sum_squares + 1e-06))
    scaled = clip_scale * wide
    moment1 = beta_one * new_first + (1.0 - beta_one) * scaled
    moment2 = beta_two * new_second + (1.0 - beta_two) * scaled * scaled
    update = moment1 / correct_one / (jnp.sqrt(moment2 / correct_two) + adam_eps)
    master = new_master - learning_rate * (update + weight_decay * new_master)
    return (master, moment1, moment2)


def solution(mesh):
    in_specs = (
        P("dp", "tensor"),
        P("dp", "tensor"),
        P("dp", "tensor"),
        P("dp", "tensor"),
        P("dp", None),
        P("dp", None),
    )
    out_specs = (P("dp", "tensor"), P("dp", "tensor"), P("dp", "tensor"))
    return jax.shard_map(
        per_device, mesh=mesh, in_specs=in_specs, out_specs=out_specs, check_vma=False
    )
```
